256 devices in a mesh: mkt: 8 (over z), prod: 2 (over core), draw: 16 (over y, x).
Axes of the slice: x: 4, y: 4, z: 8, core: 2. Of those that a mesh axis runs over, the one named last changes fastest.
Arguments:
- start_utility: float32 [2048, 256], P('mkt', 'prod'), may hold values from -5 to -2
- log_shares: float32 [2048, 256], P('mkt', 'prod'), may hold values from -9 to -5
- characteristics: float32 [2048, 8, 256], P('mkt', None, 'prod'), may hold values from -2.5 to 2.5
- coef_scale: float32 [8], replicated, may hold values from 0.1 to 0.3
- taste_draws: float32 [2048, 8, 2048], P('mkt', None, 'draw'), may hold values from -2.5 to 2.5
Outputs:
- mean_utility: float32 [2048, 256], P('mkt', 'prod')
- step_norms: float32 [2], replicated
The draws below stay inside these ranges and needn't reach their ends.
All inputs are finite; a program needn't handle non-finite values.
Results may differ from the reference program's by a relative error of at most 0.0001.
Values sent between devices are 32-bit elements; how exact they have to be, the bound alone decides.
No kernel may reach another device: no remote copies, remote signals or barrier semaphores. Data moves between devices by JAX's collectives and lax.ppermute only.
A program may use at most 64 MiB of HBM per device.

```python
import math
import jax
import jax.numpy as jnp
from jax import lax

J = 256
R = 2048
K = 8
ITERS = 2
M = 2048


def block_levels(stream_key, shape, split, low, high):
    level, own = 1.0, jax.random.fold_in(stream_key, 6)
    for position, shards_of in split:
        draws = jnp.exp(jax.random.uniform(jax.random.fold_in(own, position), (shards_of,), jnp.float32, low / len(split), high / len(split)))
        level = level * jnp.repeat(draws, shape[position] // shards_of).reshape([-1 if axis == position else 1 for axis in range(len(shape))])
    return level


def gaussian(key, dims, width, bound, split=(), kind=jnp.bfloat16):
    level = block_levels(key, dims, split, -0.22, 0.18) if split else 1.0
    drawn = jax.random.normal(key, dims, jnp.float32) * width * level
    return jnp.minimum(jnp.maximum(drawn, -bound), bound).astype(kind)


def setup_inputs(seed: int = 0) -> dict:
    splits = jax.random.split(jax.random.key(seed), 6)
    return {
        "start_utility": jnp.clip(-5.0 + 3.0 * jax.random.uniform(splits[0], (M, J), jnp.float32) ** block_levels(splits[0], (M, J), ((0, 8), (1, 2)), -0.2, 0.2), -5.0, -2.0),
        "log_shares": jnp.clip(-9.0 + 4.0 * jax.random.uniform(splits[1], (M, J), jnp.float32) ** block_levels(splits[1], (M, J), ((0, 8), (1, 2)), -0.2, 0.2), -9.0, -5.0),
        "characteristics": gaussian(splits[2], (M, K, J), 1.0, 2.5, ((0, 8), (2, 2)), jnp.float32),
        "coef_scale": jnp.clip(jnp.exp(jax.random.uniform(splits[3], (K,), jnp.float32, math.log(0.1), math.log(0.3))), 0.1, 0.3),
        "taste_draws": gaussian(splits[4], (M, K, R), 1.0, 2.5, ((0, 8), (2, 16)), jnp.float32),
    }


def reference(start_utility, log_shares, characteristics, coef_scale, taste_draws):
    scaled = taste_draws * coef_scale[None, :, None]
    block_size = math.gcd(M, 16)
    block_count = M // block_size

    def predict(utility):

        def market_block(inputs):
            chars_part, scaled_part, util_part = inputs
            spread = jnp.einsum('mkj,mkr->mjr', chars_part, scaled_part, precision=lax.Precision.HIGHEST)
            weight = jnp.exp(util_part[:, :, None] + spread)
            denominator = 1.0 + lax.optimization_barrier(jnp.sum(weight, axis=1, keepdims=True))
            return lax.optimization_barrier(jnp.sum(weight / denominator, axis=2)) / R
        result = lax.map(market_block, (characteristics.reshape(block_count, block_size, K, J), scaled.reshape(block_count, block_size, K, R), utility.reshape(block_count, block_size, J)))
        return result.reshape(M, J)
    utility = start_utility
    norm_list = []
    for iteration in range(ITERS):
        predicted = predict(utility)
        updated = utility + log_shares - jnp.log(predicted)
        change = updated - utility
        norm_list.append(jnp.sqrt(jnp.mean(change * change) + 1e-06))
        utility = updated
    return (utility, jnp.stack(norm_list))
```

```python
import math

import jax
import jax.numpy as jnp
from jax import lax
from jax.experimental import pallas as pl
from jax.experimental.pallas import tpu as pltpu
from jax.sharding import PartitionSpec as P

R = 2048
LOG2E = math.log2(math.e)
LANES = 128
SUBLANES = 8


def rounded(x):
    return x.astype(jnp.bfloat16).astype(jnp.float32)


def first_rows(rows, length):
    width = rows[0].shape[-1]
    index = lax.broadcasted_iota(jnp.int32, (length, width), 0)
    out = jnp.zeros((length, width), jnp.float32)
    for position, row in enumerate(rows):
        out = jnp.where(index == position, jnp.broadcast_to(row, (length, width)), out)
    return out


def three_parts(x):
    high = rounded(x)
    middle = rounded(x - high)
    return high, middle, x - high - middle


def by_first(a, b):
    return lax.dot_general(a, b, (((0,), (0,)), ((), ())), preferred_element_type=jnp.float32)


def by_last(a, b):
    return lax.dot_general(a, b, (((1,), (1,)), ((), ())), preferred_element_type=jnp.float32)


def contraction_kernel(core_ref, coef_ref, own_ref, other_ref, taste_ref, out_ref, weight_ref, inverse_ref, share_ref, factor_ref):
    markets = own_ref.shape[0] // 10
    coefs = 8
    chips = taste_ref.shape[0]
    groups = 2 * LANES // SUBLANES
    core = core_ref[0]

    def part(first, count):
        return jnp.concatenate([own_ref[pl.ds(first, count)], other_ref[pl.ds(first, count)]], axis=1)

    utility = part(8 * markets, markets)
    shares = part(9 * markets, markets)

    coef = jnp.concatenate([jnp.full((1, 2 * LANES), coef_ref[k] * LOG2E, jnp.float32) for k in range(coefs)], axis=0)
    ones = first_rows([jnp.ones((1, 2 * LANES), jnp.float32)] * 3, SUBLANES)

    def all_sublanes(x):
        for shift in (4, 2, 1):
            x = x + pltpu.roll(x, shift, 0)
        return x

    for m in range(markets):
        chars = part(m * coefs, coefs) * coef
        high = rounded(chars)
        base = first_rows(three_parts(utility[m : m + 1] * LOG2E), SUBLANES)
        left = jnp.concatenate([high, high, chars - high, base], axis=0).astype(jnp.bfloat16)
        for t in range(0, chips, 2):
            taste = jnp.concatenate([taste_ref[t, m], taste_ref[t + 1, m]], axis=1)
            taste_high = rounded(taste)
            right = jnp.concatenate([taste_high, taste - taste_high, taste_high, ones], axis=0).astype(jnp.bfloat16)
            weight = jnp.exp2(by_first(left, right))
            for half in range(2):
                piece = weight[:, half * LANES : (half + 1) * LANES]
                weight_ref[m, t + half] = piece
                total = jnp.sum(piece.reshape(groups, SUBLANES, LANES), axis=0)
                inverse_ref[m, t + half] = 1.0 / (1.0 + all_sublanes(total))

    def share_pass():
        predicted = jnp.zeros((SUBLANES, 2 * LANES), jnp.float32)
        row = lax.broadcasted_iota(jnp.int32, (SUBLANES, LANES), 0)

        def one(m, carry):
            inverse = [inverse_ref[m, t] for t in range(chips)]
            for g in range(groups):
                rows = pl.ds(g * SUBLANES, SUBLANES)
                terms = [weight_ref[m, t, rows] * inverse[t] for t in range(chips)]
                while len(terms) > 1:
                    terms = [a + b for a, b in zip(terms[::2], terms[1::2])]
                share_ref[m, rows] = terms[0]
            return carry

        lax.fori_loop(0, markets, one, 0)
        for m in range(markets):
            pick = jnp.where(row == m, 1.0, 0.0).astype(jnp.bfloat16)
            for piece in three_parts(share_ref[m]):
                predicted = predicted + by_last(pick, piece.astype(jnp.bfloat16))
        return predicted

    first_change = shares - jnp.log(share_pass() * (1.0 / R))
    factor = jnp.exp(first_change)
    for m in range(markets):
        left = first_rows(three_parts(factor[m : m + 1]), 2 * SUBLANES).astype(jnp.bfloat16)
        factor_ref[m] = by_first(left, jnp.ones((2 * SUBLANES, LANES), jnp.bfloat16))

    def total_pass(m, carry):
        totals = [jnp.zeros((SUBLANES, LANES), jnp.float32)] * chips
        for g in range(groups):
            rows = pl.ds(g * SUBLANES, SUBLANES)
            scale = factor_ref[m, rows]
            totals = [total + weight_ref[m, t, rows] * scale for t, total in enumerate(totals)]
        for t in range(chips):
            inverse_ref[m, t] = 1.0 / (1.0 + all_sublanes(totals[t]))
        return carry

    lax.fori_loop(0, markets, total_pass, 0)

    second_change = shares - jnp.log(factor * share_pass() * (1.0 / R))
    result = utility + first_change + second_change

    squares = []
    for change in (first_change, second_change):
        square = change * change
        square = square[:, :LANES] + square[:, LANES:]
        squares.append(jnp.sum(square, axis=0, keepdims=True))
    squares = first_rows(squares, SUBLANES)
    for half, place in enumerate((core, 1 - core)):
        block = jnp.concatenate([result[:, half * LANES : (half + 1) * LANES], squares], axis=0)
        out_ref[pl.ds(place * chips, chips)] = jnp.broadcast_to(block, (chips, 2 * SUBLANES, LANES))


def contraction(core, coef_scale, own, other, taste):
    chips, markets, coefs, lanes = taste.shape
    smem = pl.BlockSpec(memory_space=pltpu.SMEM)
    vmem = pl.BlockSpec(memory_space=pltpu.VMEM)
    return pl.pallas_call(
        contraction_kernel,
        out_shape=jax.ShapeDtypeStruct((2 * chips, 2 * SUBLANES, LANES), jnp.float32),
        in_specs=[smem, smem, vmem, vmem, vmem],
        out_specs=vmem,
        scratch_shapes=[
            pltpu.VMEM((markets, chips, 2 * LANES, LANES), jnp.float32),
            pltpu.VMEM((markets, chips, SUBLANES, LANES), jnp.float32),
            pltpu.VMEM((markets, 2 * LANES, LANES), jnp.float32),
            pltpu.VMEM((markets, 2 * LANES, LANES), jnp.float32),
        ],
        compiler_params=pltpu.CompilerParams(vmem_limit_bytes=48 * 1024 * 1024),
    )(core, coef_scale, own, other, taste)


def shards(start_utility, log_shares, characteristics, coef_scale, taste_draws):
    markets, coefs, _ = characteristics.shape
    cores, chips = lax.axis_size("prod"), lax.axis_size("draw")
    own_markets = markets // (cores * chips)
    core, chip = lax.axis_index("prod"), lax.axis_index("draw")

    half = lax.dynamic_slice_in_dim(taste_draws, core * (markets // cores), markets // cores, 0)
    taste = lax.all_to_all(half.reshape(chips, own_markets, coefs, LANES), "draw", 0, 0, tiled=True)

    def packed(first):
        chars = lax.dynamic_slice_in_dim(characteristics, first, own_markets, 0).reshape(-1, LANES)
        utility = lax.dynamic_slice_in_dim(start_utility, first, own_markets, 0)
        shares = lax.dynamic_slice_in_dim(log_shares, first, own_markets, 0)
        return jnp.concatenate([chars, utility, shares], axis=0)

    place = chip * own_markets
    own = packed(core * (markets // cores) + place)
    other = lax.ppermute(packed((1 - core) * (markets // cores) + place), "prod", [(0, 1), (1, 0)])

    blocks = contraction(core.reshape(1), coef_scale, own, other, taste)
    blocks = lax.all_to_all(blocks, ("prod", "draw"), 0, 0, tiled=True)
    utility = blocks[:, :own_markets].reshape(markets, LANES)
    squares = jnp.sum(blocks[:, own_markets : own_markets + 2], axis=0)
    planes = lax.axis_size("mkt")
    step = 1
    while step < planes:
        squares = squares + lax.ppermute(squares, "mkt", [(i, i ^ step) for i in range(planes)])
        step *= 2
    cells = planes * markets * cores * LANES
    return utility, jnp.sqrt(jnp.sum(squares, axis=1) / cells + 1e-06)


def solution(mesh):
    return jax.shard_map(
        shards,
        mesh=mesh,
        in_specs=(
            P("mkt", "prod"),
            P("mkt", "prod"),
            P("mkt", None, "prod"),
            P(),
            P("mkt", None, "draw"),
        ),
        out_specs=(P("mkt", "prod"), P()),
        check_vma=False,
    )
```

```python
import math

import jax
import jax.numpy as jnp
from jax import lax
from jax.experimental import pallas as pl
from jax.experimental.pallas import tpu as pltpu
from jax.sharding import PartitionSpec as P

R = 2048
LOG2E = math.log2(math.e)
LANES = 128
SUBLANES = 8


def rounded(x):
    return x.astype(jnp.bfloat16).astype(jnp.float32)


def first_rows(rows, length):
    width = rows[0].shape[-1]
    index = lax.broadcasted_iota(jnp.int32, (length, width), 0)
    out = jnp.zeros((length, width), jnp.float32)
    for position, row in enumerate(rows):
        out = jnp.where(index == position, jnp.broadcast_to(row, (length, width)), out)
    return out


def three_parts(x):
    high = rounded(x)
    middle = rounded(x - high)
    return high, middle, x - high - middle


def by_first(a, b):
    return lax.dot_general(a, b, (((0,), (0,)), ((), ())), preferred_element_type=jnp.float32)


def all_sublanes(x):
    for shift in (4, 2, 1):
        x = x + pltpu.roll(x, shift, 0)
    return x


def added(terms):
    while len(terms) > 1:
        terms = [a + b for a, b in zip(terms[::2], terms[1::2])]
    return terms[0]


def contraction_kernel(coef_ref, own_ref, other_ref, taste_ref, out_ref, weight_ref, inverse_ref, share_ref, factor_ref, left_ref, row_ref):
    markets = own_ref.shape[0] // 10
    coefs = 8
    chips = taste_ref.shape[0]
    groups = 2 * LANES // SUBLANES
    slices = chips // 2

    def part(first, count):
        return jnp.concatenate([own_ref[pl.ds(first, count)], other_ref[pl.ds(first, count)]], axis=1)

    coef = jnp.concatenate([jnp.full((1, 2 * LANES), coef_ref[k] * LOG2E, jnp.float32) for k in range(coefs)], axis=0)
    ones = first_rows([jnp.ones((1, 2 * LANES), jnp.float32)] * 3, SUBLANES)

    def left_of(m):
        chars = part(m * coefs, coefs) * coef
        high = rounded(chars)
        base = first_rows(three_parts(part(8 * markets + m, 1) * LOG2E), SUBLANES)
        left_ref[m] = jnp.concatenate([high, high, chars - high, base], axis=0).astype(jnp.bfloat16)

    def weigh(m, q):
        taste = jnp.concatenate([taste_ref[2 * q, m], taste_ref[2 * q + 1, m]], axis=1)
        taste_high = rounded(taste)
        right = jnp.concatenate([taste_high, taste - taste_high, taste_high, ones], axis=0).astype(jnp.bfloat16)
        weight = jnp.exp2(by_first(left_ref[m], right))
        for half in range(2):
            piece = weight[:, half * LANES : (half + 1) * LANES]
            weight_ref[m, 2 * q + half] = piece
            total = jnp.sum(piece.reshape(groups, SUBLANES, LANES), axis=0)
            inverse_ref[m, 2 * q + half] = 1.0 / (1.0 + all_sublanes(total))

    def share(m, q):
        inverse = [inverse_ref[m, t] for t in range(chips)]
        for g in range(q * groups // slices, (q + 1) * groups // slices):
            rows = pl.ds(g * SUBLANES, SUBLANES)
            share_ref[m, rows] = added([weight_ref[m, t, rows] * inverse[t] for t in range(chips)])

    def predicted(m):
        return jnp.sum(share_ref[m].T, axis=0, keepdims=True) * (1.0 / R)

    def first_end(m):
        change = part(9 * markets + m, 1) - jnp.log(predicted(m))
        factor = jnp.exp(change)
        row_ref[0, pl.ds(m, 1)] = change
        row_ref[1, pl.ds(m, 1)] = factor
        factor_ref[m] = jnp.broadcast_to(factor, (LANES, 2 * LANES)).T

    def weigh_again(m, q):
        totals = [[] for _ in range(2)]
        for g in range(groups):
            rows = pl.ds(g * SUBLANES, SUBLANES)
            scale = factor_ref[m, rows]
            for half in range(2):
                term = weight_ref[m, 2 * q + half, rows] * scale
                if g < 2:
                    totals[half].append(term)
                else:
                    totals[half][g % 2] = totals[half][g % 2] + term
        for half in range(2):
            inverse_ref[m, 2 * q + half] = 1.0 / (1.0 + all_sublanes(added(totals[half])))

    def second_end(m):
        row_ref[2, pl.ds(m, 1)] = predicted(m)

    for stage in range(markets + 3):
        a, b, c, d = (stage - lag if 0 <= stage - lag < markets else None for lag in range(4))
        if a is not None:
            left_of(a)
        for q in range(slices):
            if a is not None:
                weigh(a, q)
            if b is not None:
                share(b, q)
            if c is not None:
                weigh_again(c, q)
            if d is not None:
                share(d, q)
        if b is not None:
            first_end(b)
        if d is not None:
            second_end(d)

    first_change = row_ref[0]
    second_change = part(9 * markets, markets) - jnp.log(row_ref[1] * row_ref[2])
    result = part(8 * markets, markets) + first_change + second_change
    squares = []
    for change in (first_change, second_change):
        square = change * change
        square = square[:, :LANES] + square[:, LANES:]
        squares.append(jnp.sum(square, axis=0, keepdims=True))
    block = jnp.concatenate([result[:, :LANES], result[:, LANES:], first_rows(squares, SUBLANES)], axis=0)
    out_ref[...] = jnp.broadcast_to(block, (chips, 3 * SUBLANES, LANES))


def contraction(coef_scale, own, other, taste):
    chips, markets, _, _ = taste.shape
    smem = pl.BlockSpec(memory_space=pltpu.SMEM)
    vmem = pl.BlockSpec(memory_space=pltpu.VMEM)
    return pl.pallas_call(
        contraction_kernel,
        out_shape=jax.ShapeDtypeStruct((chips, 3 * SUBLANES, LANES), jnp.float32),
        in_specs=[smem, vmem, vmem, vmem],
        out_specs=vmem,
        scratch_shapes=[
            pltpu.VMEM((markets, chips, 2 * LANES, LANES), jnp.float32),
            pltpu.VMEM((markets, chips, SUBLANES, LANES), jnp.float32),
            pltpu.VMEM((markets, 2 * LANES, LANES), jnp.float32),
            pltpu.VMEM((markets, 2 * LANES, LANES), jnp.float32),
            pltpu.VMEM((markets, 4 * SUBLANES, 2 * LANES), jnp.bfloat16),
            pltpu.VMEM((3, markets, 2 * LANES), jnp.float32),
        ],
        compiler_params=pltpu.CompilerParams(vmem_limit_bytes=40 * 1024 * 1024),
    )(coef_scale, own, other, taste)


def take_half_kernel(core_ref, whole_ref, half_ref, sem):
    count = half_ref.shape[0]
    copy = pltpu.make_async_copy(whole_ref.at[pl.ds(core_ref[0] * count, count)], half_ref, sem)
    copy.start()
    copy.wait()


def take_half(core, whole, count):
    return pl.pallas_call(
        take_half_kernel,
        out_shape=jax.ShapeDtypeStruct((count, *whole.shape[1:]), whole.dtype),
        in_specs=[pl.BlockSpec(memory_space=pltpu.SMEM), pl.BlockSpec(memory_space=pltpu.HBM)],
        out_specs=pl.BlockSpec(memory_space=pltpu.VMEM),
        scratch_shapes=[pltpu.SemaphoreType.DMA(())],
    )(core.reshape(1), whole)


def shards(start_utility, log_shares, characteristics, coef_scale, taste_draws):
    markets, coefs, _ = characteristics.shape
    cores, chips, planes = lax.axis_size("prod"), lax.axis_size("draw"), lax.axis_size("mkt")
    half = markets // cores
    own_markets = half // chips
    core, chip = lax.axis_index("prod"), lax.axis_index("draw")

    taste = take_half(core, taste_draws, half).reshape(chips, own_markets, coefs, LANES)
    taste = lax.all_to_all(taste, "draw", 0, 0, tiled=True)

    def packed(first):
        chars = lax.dynamic_slice_in_dim(characteristics, first, own_markets, 0).reshape(-1, LANES)
        utility = lax.dynamic_slice_in_dim(start_utility, first, own_markets, 0)
        shares = lax.dynamic_slice_in_dim(log_shares, first, own_markets, 0)
        return jnp.concatenate([chars, utility, shares], axis=0)

    swap = [(0, 1), (1, 0)]
    own = packed(core * half + chip * own_markets)
    other = lax.ppermute(packed((1 - core) * half + chip * own_markets), "prod", swap)

    blocks = contraction(coef_scale, own, other, taste)
    blocks = lax.all_to_all(blocks, "draw", 0, 0, tiled=True)

    squares = jnp.sum(blocks[:, 2 * own_markets : 2 * own_markets + 2], axis=0)
    squares = jnp.broadcast_to(squares, (planes * cores, 2, LANES))
    squares = lax.all_to_all(squares, ("mkt", "prod"), 0, 0, tiled=True)
    kept = blocks[:, :own_markets].reshape(half, LANES)
    given = blocks[:, own_markets : 2 * own_markets].reshape(half, LANES)
    given = lax.ppermute(given, "prod", swap)
    first = core == 0
    utility = jnp.concatenate([jnp.where(first, kept, given), jnp.where(first, given, kept)], axis=0)
    cells = planes * markets * cores * LANES
    return utility, jnp.sqrt(jnp.sum(squares, axis=(0, 2)) / cells + 1e-06)


def solution(mesh):
    return jax.shard_map(
        shards,
        mesh=mesh,
        in_specs=(
            P("mkt", "prod"),
            P("mkt", "prod"),
            P("mkt", None, "prod"),
            P(),
            P("mkt", None, "draw"),
        ),
        out_specs=(P("mkt", "prod"), P()),
        check_vma=False,
    )
```

```python
import math

import jax
import jax.numpy as jnp
from jax import lax
from jax.experimental import pallas as pl
from jax.experimental.pallas import tpu as pltpu
from jax.sharding import PartitionSpec as P

R = 2048
LOG2E = math.log2(math.e)
LANES = 128
SUBLANES = 8


def rounded(x):
    return x.astype(jnp.bfloat16).astype(jnp.float32)


def first_rows(rows, length):
    width = rows[0].shape[-1]
    index = lax.broadcasted_iota(jnp.int32, (length, width), 0)
    out = jnp.zeros((length, width), jnp.float32)
    for position, row in enumerate(rows):
        out = jnp.where(index == position, jnp.broadcast_to(row, (length, width)), out)
    return out


def three_parts(x):
    high = rounded(x)
    middle = rounded(x - high)
    return high, middle, x - high - middle


def by_first(a, b):
    return lax.dot_general(a, b, (((0,), (0,)), ((), ())), preferred_element_type=jnp.float32)


def all_sublanes(x):
    for shift in (4, 2, 1):
        x = x + pltpu.roll(x, shift, 0)
    return x


def added(terms):
    while len(terms) > 1:
        terms = [a + b for a, b in zip(terms[::2], terms[1::2])]
    return terms[0]


def contraction_kernel(coef_ref, own_ref, other_ref, taste_ref, out_ref, weight_ref, inverse_ref, share_ref, factor_ref, left_ref, row_ref):
    markets = own_ref.shape[0] // 10
    coefs = 8
    chips = taste_ref.shape[0]
    groups = 2 * LANES // SUBLANES
    slices = chips // 2

    def part(first, count):
        return jnp.concatenate([own_ref[pl.ds(first, count)], other_ref[pl.ds(first, count)]], axis=1)

    coef = jnp.concatenate([jnp.full((1, 2 * LANES), coef_ref[k] * LOG2E, jnp.float32) for k in range(coefs)], axis=0)
    ones = first_rows([jnp.ones((1, 2 * LANES), jnp.float32)] * 3, SUBLANES)

    def left_of(m):
        chars = part(m * coefs, coefs) * coef
        high = rounded(chars)
        base = first_rows(three_parts(part(8 * markets + m, 1) * LOG2E), SUBLANES)
        left_ref[m] = jnp.concatenate([high, high, chars - high, base], axis=0).astype(jnp.bfloat16)

    def weigh(m, q):
        taste = jnp.concatenate([taste_ref[2 * q, m], taste_ref[2 * q + 1, m]], axis=1)
        taste_high = rounded(taste)
        right = jnp.concatenate([taste_high, taste - taste_high, taste_high, ones], axis=0).astype(jnp.bfloat16)
        weight = jnp.exp2(by_first(left_ref[m], right))
        for half in range(2):
            piece = weight[:, half * LANES : (half + 1) * LANES]
            weight_ref[m, 2 * q + half] = piece
            total = jnp.sum(piece.reshape(groups, SUBLANES, LANES), axis=0)
            inverse_ref[m, 2 * q + half] = 1.0 / (1.0 + all_sublanes(total))

    def share(m, q):
        inverse = [inverse_ref[m, t] for t in range(chips)]
        for g in range(q * groups // slices, (q + 1) * groups // slices):
            rows = pl.ds(g * SUBLANES, SUBLANES)
            share_ref[m, rows] = added([weight_ref[m, t, rows] * inverse[t] for t in range(chips)])

    def predicted(m):
        return jnp.sum(share_ref[m].T, axis=0, keepdims=True) * (1.0 / R)

    def first_end(m):
        change = part(9 * markets + m, 1) - jnp.log(predicted(m))
        factor = jnp.exp(change)
        row_ref[0, pl.ds(m, 1)] = change
        row_ref[1, pl.ds(m, 1)] = factor
        factor_ref[m] = jnp.broadcast_to(factor, (LANES, 2 * LANES)).T

    again = {}

    def weigh_again(m, q):
        totals = again.setdefault(m, [None] * chips)
        for g in range(q * groups // slices, (q + 1) * groups // slices):
            rows = pl.ds(g * SUBLANES, SUBLANES)
            scale = factor_ref[m, rows]
            for t in range(chips):
                term = weight_ref[m, t, rows] * scale
                totals[t] = term if totals[t] is None else totals[t] + term
        if q == slices - 1:
            for t in range(chips):
                inverse_ref[m, t] = 1.0 / (1.0 + all_sublanes(totals[t]))

    def second_end(m):
        row_ref[2, pl.ds(m, 1)] = predicted(m)

    for stage in range(markets + 3):
        a, b, c, d = (stage - lag if 0 <= stage - lag < markets else None for lag in range(4))
        if a is not None:
            left_of(a)
        for q in range(slices):
            if a is not None:
                weigh(a, q)
            if b is not None:
                share(b, q)
            if c is not None:
                weigh_again(c, q)
            if d is not None:
                share(d, q)
        if b is not None:
            first_end(b)
        if d is not None:
            second_end(d)

    first_change = row_ref[0]
    second_change = part(9 * markets, markets) - jnp.log(row_ref[1] * row_ref[2])
    result = part(8 * markets, markets) + first_change + second_change
    squares = []
    for change in (first_change, second_change):
        square = change * change
        square = square[:, :LANES] + square[:, LANES:]
        squares.append(jnp.sum(square, axis=0, keepdims=True))
    block = jnp.concatenate([result[:, :LANES], result[:, LANES:], first_rows(squares, SUBLANES)], axis=0)
    out_ref[...] = jnp.broadcast_to(block, (chips, 3 * SUBLANES, LANES))


def contraction(coef_scale, own, other, taste):
    chips, markets, _, _ = taste.shape
    smem = pl.BlockSpec(memory_space=pltpu.SMEM)
    vmem = pl.BlockSpec(memory_space=pltpu.VMEM)
    return pl.pallas_call(
        contraction_kernel,
        out_shape=jax.ShapeDtypeStruct((chips, 3 * SUBLANES, LANES), jnp.float32),
        in_specs=[smem, vmem, vmem, vmem],
        out_specs=vmem,
        scratch_shapes=[
            pltpu.VMEM((markets, chips, 2 * LANES, LANES), jnp.float32),
            pltpu.VMEM((markets, chips, SUBLANES, LANES), jnp.float32),
            pltpu.VMEM((markets, 2 * LANES, LANES), jnp.float32),
            pltpu.VMEM((markets, 2 * LANES, LANES), jnp.float32),
            pltpu.VMEM((markets, 4 * SUBLANES, 2 * LANES), jnp.bfloat16),
            pltpu.VMEM((3, markets, 2 * LANES), jnp.float32),
        ],
        compiler_params=pltpu.CompilerParams(vmem_limit_bytes=40 * 1024 * 1024),
    )(coef_scale, own, other, taste)


def take_half_kernel(core_ref, whole_ref, half_ref, sem):
    count = half_ref.shape[0]
    copy = pltpu.make_async_copy(whole_ref.at[pl.ds(core_ref[0] * count, count)], half_ref, sem)
    copy.start()
    copy.wait()


def take_half(core, whole, count):
    return pl.pallas_call(
        take_half_kernel,
        out_shape=jax.ShapeDtypeStruct((count, *whole.shape[1:]), whole.dtype),
        in_specs=[pl.BlockSpec(memory_space=pltpu.SMEM), pl.BlockSpec(memory_space=pltpu.HBM)],
        out_specs=pl.BlockSpec(memory_space=pltpu.HBM),
        scratch_shapes=[pltpu.SemaphoreType.DMA(())],
    )(core.astype(jnp.int32).reshape(1), whole)


def shards(start_utility, log_shares, characteristics, coef_scale, taste_draws):
    markets, coefs, _ = characteristics.shape
    cores, chips, planes = lax.axis_size("prod"), lax.axis_size("draw"), lax.axis_size("mkt")
    half = markets // cores
    own_markets = half // chips
    core, chip = (lax.axis_index(axis).astype(jnp.uint32) for axis in ("prod", "draw"))

    taste = take_half(core, taste_draws, half).reshape(chips, own_markets, coefs, LANES)
    taste = lax.all_to_all(taste, "draw", 0, 0, tiled=True)

    def packed(first):
        chars = lax.dynamic_slice_in_dim(characteristics, first, own_markets, 0).reshape(-1, LANES)
        utility = lax.dynamic_slice_in_dim(start_utility, first, own_markets, 0)
        shares = lax.dynamic_slice_in_dim(log_shares, first, own_markets, 0)
        return jnp.concatenate([chars, utility, shares], axis=0)

    swap = [(0, 1), (1, 0)]
    own = packed(core * half + chip * own_markets)
    other = lax.ppermute(packed((1 - core) * half + chip * own_markets), "prod", swap)

    blocks = contraction(coef_scale, own, other, taste)
    blocks = lax.all_to_all(blocks, "draw", 0, 0, tiled=True)

    squares = jnp.sum(blocks[:, 2 * own_markets : 2 * own_markets + 2], axis=0)
    squares = jnp.broadcast_to(squares, (planes * cores, 2, LANES))
    squares = lax.all_to_all(squares, ("mkt", "prod"), 0, 0, tiled=True)
    kept = blocks[:, :own_markets].reshape(half, LANES)
    given = blocks[:, own_markets : 2 * own_markets].reshape(half, LANES)
    given = lax.ppermute(given, "prod", swap)
    utility = jnp.zeros((markets, LANES), jnp.float32)
    utility = lax.dynamic_update_slice_in_dim(utility, kept, core * half, 0)
    utility = lax.dynamic_update_slice_in_dim(utility, given, (1 - core) * half, 0)
    cells = planes * markets * cores * LANES
    return utility, jnp.sqrt(jnp.sum(squares, axis=(0, 2)) / cells + 1e-06)


def solution(mesh):
    return jax.shard_map(
        shards,
        mesh=mesh,
        in_specs=(
            P("mkt", "prod"),
            P("mkt", "prod"),
            P("mkt", None, "prod"),
            P(),
            P("mkt", None, "draw"),
        ),
        out_specs=(P("mkt", "prod"), P()),
        check_vma=False,
    )
```

```python
import math

import jax
import jax.numpy as jnp
from jax import lax
from jax.experimental import pallas as pl
from jax.experimental.pallas import tpu as pltpu
from jax.sharding import PartitionSpec as P

R = 2048
LOG2E = math.log2(math.e)
LANES = 128
SUBLANES = 8


def rounded(x):
    return x.astype(jnp.bfloat16).astype(jnp.float32)


def first_rows(rows, length):
    width = rows[0].shape[-1]
    index = lax.broadcasted_iota(jnp.int32, (length, width), 0)
    out = jnp.zeros((length, width), jnp.float32)
    for position, row in enumerate(rows):
        out = jnp.where(index == position, jnp.broadcast_to(row, (length, width)), out)
    return out


def three_parts(x):
    high = rounded(x)
    middle = rounded(x - high)
    return high, middle, x - high - middle


def by_first(a, b):
    return lax.dot_general(a, b, (((0,), (0,)), ((), ())), preferred_element_type=jnp.float32)


def all_sublanes(x):
    for shift in (4, 2, 1):
        x = x + pltpu.roll(x, shift, 0)
    return x


def added(terms):
    while len(terms) > 1:
        terms = [a + b for a, b in zip(terms[::2], terms[1::2])]
    return terms[0]


def contraction_kernel(own_ref, other_ref, taste_ref, out_ref, weight_ref, inverse_ref, share_ref, factor_ref, left_ref, row_ref):
    coefs = 8
    markets = other_ref.shape[0] // (coefs + 2)
    chips = taste_ref.shape[0]
    groups = 2 * LANES // SUBLANES
    slices = chips // 2

    def part(first, count):
        return jnp.concatenate([own_ref[pl.ds(first, count)], other_ref[pl.ds(first, count)]], axis=1)

    coef = own_ref[pl.ds((coefs + 2) * markets, coefs)] * LOG2E
    coef = jnp.concatenate([coef, coef], axis=1)
    ones = first_rows([jnp.ones((1, 2 * LANES), jnp.float32)] * 3, SUBLANES)

    def left_of(m):
        chars = part(m * coefs, coefs) * coef
        high = rounded(chars)
        base = first_rows(three_parts(part(8 * markets + m, 1) * LOG2E), SUBLANES)
        left_ref[m] = jnp.concatenate([high, high, chars - high, base], axis=0).astype(jnp.bfloat16)

    def weigh(m, q):
        taste = jnp.concatenate([taste_ref[2 * q, m], taste_ref[2 * q + 1, m]], axis=1)
        taste_high = rounded(taste)
        right = jnp.concatenate([taste_high, taste - taste_high, taste_high, ones], axis=0).astype(jnp.bfloat16)
        weight = jnp.exp2(by_first(left_ref[m], right))
        for half in range(2):
            piece = weight[:, half * LANES : (half + 1) * LANES]
            weight_ref[m, 2 * q + half] = piece
            total = jnp.sum(piece.reshape(groups, SUBLANES, LANES), axis=0)
            inverse_ref[m, 2 * q + half] = 1.0 / (1.0 + all_sublanes(total))

    def share(m, q):
        inverse = [inverse_ref[m, t] for t in range(chips)]
        for g in range(q * groups // slices, (q + 1) * groups // slices):
            rows = pl.ds(g * SUBLANES, SUBLANES)
            share_ref[m, rows] = added([weight_ref[m, t, rows] * inverse[t] for t in range(chips)])

    def predicted(m):
        return jnp.sum(share_ref[m].T, axis=0, keepdims=True) * (1.0 / R)

    def first_end(m):
        change = part(9 * markets + m, 1) - jnp.log(predicted(m))
        factor = jnp.exp(change)
        row_ref[0, pl.ds(m, 1)] = change
        row_ref[1, pl.ds(m, 1)] = factor
        factor_ref[m] = jnp.broadcast_to(factor, (LANES, 2 * LANES)).T

    again = {}

    def weigh_again(m, q):
        totals = again.setdefault(m, [None] * chips)
        for g in range(q * groups // slices, (q + 1) * groups // slices):
            rows = pl.ds(g * SUBLANES, SUBLANES)
            scale = factor_ref[m, rows]
            for t in range(chips):
                term = weight_ref[m, t, rows] * scale
                totals[t] = term if totals[t] is None else totals[t] + term
        if q == slices - 1:
            for t in range(chips):
                inverse_ref[m, t] = 1.0 / (1.0 + all_sublanes(totals[t]))

    def second_end(m):
        row_ref[2, pl.ds(m, 1)] = predicted(m)

    for stage in range(markets + 3):
        a, b, c, d = (stage - lag if 0 <= stage - lag < markets else None for lag in range(4))
        if a is not None:
            left_of(a)
        for q in range(slices):
            if a is not None:
                weigh(a, q)
            if b is not None:
                share(b, q)
            if c is not None:
                weigh_again(c, q)
            if d is not None:
                share(d, q)
        if b is not None:
            first_end(b)
        if d is not None:
            second_end(d)

    first_change = row_ref[0]
    second_change = part(9 * markets, markets) - jnp.log(row_ref[1] * row_ref[2])
    result = part(8 * markets, markets) + first_change + second_change
    squares = []
    for change in (first_change, second_change):
        square = change * change
        square = square[:, :LANES] + square[:, LANES:]
        squares.append(jnp.sum(square, axis=0, keepdims=True))
    block = jnp.concatenate([result[:, :LANES], result[:, LANES:], first_rows(squares, SUBLANES)], axis=0)
    out_ref[...] = jnp.broadcast_to(block, (chips, 3 * SUBLANES, LANES))


def contraction(own, other, taste):
    chips, markets, _, _ = taste.shape
    vmem = pl.BlockSpec(memory_space=pltpu.VMEM)
    return pl.pallas_call(
        contraction_kernel,
        out_shape=jax.ShapeDtypeStruct((chips, 3 * SUBLANES, LANES), jnp.float32),
        in_specs=[vmem, vmem, vmem],
        out_specs=vmem,
        scratch_shapes=[
            pltpu.VMEM((markets, chips, 2 * LANES, LANES), jnp.float32),
            pltpu.VMEM((markets, chips, SUBLANES, LANES), jnp.float32),
            pltpu.VMEM((markets, 2 * LANES, LANES), jnp.float32),
            pltpu.VMEM((markets, 2 * LANES, LANES), jnp.float32),
            pltpu.VMEM((markets, 4 * SUBLANES, 2 * LANES), jnp.bfloat16),
            pltpu.VMEM((3, markets, 2 * LANES), jnp.float32),
        ],
        compiler_params=pltpu.CompilerParams(vmem_limit_bytes=40 * 1024 * 1024),
    )(own, other, taste)


def take_half_kernel(whole_ref, half_ref, staging_ref, read_sems, write_sems):
    pieces = read_sems.shape[0]
    count = half_ref.shape[0]
    size = count // pieces
    first = lax.axis_index("prod") * count

    def read(i):
        return pltpu.make_async_copy(whole_ref.at[pl.ds(first + i * size, size)], staging_ref.at[pl.ds(i * size, size)], read_sems.at[i])

    def write(i):
        return pltpu.make_async_copy(staging_ref.at[pl.ds(i * size, size)], half_ref.at[pl.ds(i * size, size)], write_sems.at[i])

    for i in range(pieces):
        read(i).start()
    for i in range(pieces):
        read(i).wait()
        write(i).start()
    for i in range(pieces):
        write(i).wait()


def take_half(whole, count):
    shape = (count, *whole.shape[1:])
    hbm = pl.BlockSpec(memory_space=pltpu.HBM)
    return pl.pallas_call(
        take_half_kernel,
        out_shape=jax.ShapeDtypeStruct(shape, whole.dtype),
        in_specs=[hbm],
        out_specs=hbm,
        scratch_shapes=[pltpu.VMEM(shape, whole.dtype), pltpu.SemaphoreType.DMA((4,)), pltpu.SemaphoreType.DMA((4,))],
    )(whole)


def shards(start_utility, log_shares, characteristics, coef_scale, taste_draws):
    markets, coefs, _ = characteristics.shape
    cores, chips, planes = lax.axis_size("prod"), lax.axis_size("draw"), lax.axis_size("mkt")
    half = markets // cores
    own_markets = half // chips
    core, chip = (lax.axis_index(axis).astype(jnp.uint32) for axis in ("prod", "draw"))

    taste = take_half(taste_draws, half).reshape(chips, own_markets, coefs, LANES)
    taste = lax.all_to_all(taste, "draw", 0, 0, tiled=True)

    def packed(first):
        chars = lax.dynamic_slice_in_dim(characteristics, first, own_markets, 0).reshape(-1, LANES)
        utility = lax.dynamic_slice_in_dim(start_utility, first, own_markets, 0)
        shares = lax.dynamic_slice_in_dim(log_shares, first, own_markets, 0)
        return jnp.concatenate([chars, utility, shares], axis=0)

    swap = [(0, 1), (1, 0)]
    scale = jnp.broadcast_to(coef_scale[:, None], (coefs, LANES))
    own = jnp.concatenate([packed(core * half + chip * own_markets), scale], axis=0)
    other = lax.ppermute(packed((1 - core) * half + chip * own_markets), "prod", swap)

    blocks = contraction(own, other, taste)
    blocks = lax.all_to_all(blocks, "draw", 0, 0, tiled=True)

    squares = jnp.sum(blocks[:, 2 * own_markets : 2 * own_markets + 2], axis=0)
    squares = jnp.broadcast_to(squares, (planes * cores, 2, LANES))
    squares = lax.all_to_all(squares, ("mkt", "prod"), 0, 0, tiled=True)
    kept = blocks[:, :own_markets].reshape(half, LANES)
    given = blocks[:, own_markets : 2 * own_markets].reshape(half, LANES)
    given = lax.ppermute(given, "prod", swap)
    utility = jnp.zeros((markets, LANES), jnp.float32)
    utility = lax.dynamic_update_slice_in_dim(utility, kept, core * half, 0)
    utility = lax.dynamic_update_slice_in_dim(utility, given, (1 - core) * half, 0)
    cells = planes * markets * cores * LANES
    return utility, jnp.sqrt(jnp.sum(squares, axis=(0, 2)) / cells + 1e-06)


def solution(mesh):
    return jax.shard_map(
        shards,
        mesh=mesh,
        in_specs=(
            P("mkt", "prod"),
            P("mkt", "prod"),
            P("mkt", None, "prod"),
            P(),
            P("mkt", None, "draw"),
        ),
        out_specs=(P("mkt", "prod"), P()),
        check_vma=False,
    )
```

```python
import math

import jax
import jax.numpy as jnp
from jax import lax
from jax.experimental import pallas as pl
from jax.experimental.pallas import tpu as pltpu
from jax.sharding import PartitionSpec as P

R = 2048
LOG2E = math.log2(math.e)
LANES = 128
SUBLANES = 8


def rounded(x):
    return x.astype(jnp.bfloat16).astype(jnp.float32)


def first_rows(rows, length):
    width = rows[0].shape[-1]
    index = lax.broadcasted_iota(jnp.int32, (length, width), 0)
    out = jnp.zeros((length, width), jnp.float32)
    for position, row in enumerate(rows):
        out = jnp.where(index == position, jnp.broadcast_to(row, (length, width)), out)
    return out


def three_parts(x):
    high = rounded(x)
    middle = rounded(x - high)
    return high, middle, x - high - middle


def by_first(a, b):
    return lax.dot_general(a, b, (((0,), (0,)), ((), ())), preferred_element_type=jnp.float32)


def all_sublanes(x):
    for shift in (4, 2, 1):
        x = x + pltpu.roll(x, shift, 0)
    return x


def added(terms):
    while len(terms) > 1:
        terms = [a + b for a, b in zip(terms[::2], terms[1::2])]
    return terms[0]


def contraction_kernel(gate_ref, coef_ref, own_ref, other_ref, taste_ref, out_ref, weight_ref, inverse_ref, share_ref, factor_ref, left_ref, row_ref):
    coefs = own_ref.shape[1]
    markets = own_ref.shape[0] - 2
    chips = taste_ref.shape[0]
    groups = 2 * LANES // SUBLANES
    slices = chips // 2

    def part(i):
        return jnp.concatenate([own_ref[i], other_ref[i]], axis=1)

    utility, shares = part(markets), part(markets + 1)
    square = (coefs, coefs)
    diagonal = lax.broadcasted_iota(jnp.int32, square, 0) == lax.broadcasted_iota(jnp.int32, square, 1)
    coef = jnp.where(diagonal, jnp.broadcast_to(coef_ref[...].reshape(1, coefs), square), 0.0)
    coef = jnp.broadcast_to(jnp.sum(coef, axis=1, keepdims=True) * LOG2E, (coefs, 2 * LANES))
    ones = first_rows([jnp.ones((1, 2 * LANES), jnp.float32)] * 3, SUBLANES)

    def left_of(m):
        chars = part(m) * coef
        high = rounded(chars)
        base = first_rows(three_parts(utility[m : m + 1] * LOG2E), SUBLANES)
        left_ref[m] = jnp.concatenate([high, high, chars - high, base], axis=0).astype(jnp.bfloat16)

    def weigh(m, q):
        taste = jnp.concatenate([taste_ref[2 * q, m], taste_ref[2 * q + 1, m]], axis=1)
        taste_high = rounded(taste)
        right = jnp.concatenate([taste_high, taste - taste_high, taste_high, ones], axis=0).astype(jnp.bfloat16)
        weight = jnp.exp2(by_first(left_ref[m], right))
        for half in range(2):
            piece = weight[:, half * LANES : (half + 1) * LANES]
            weight_ref[m, 2 * q + half] = piece
            total = jnp.sum(piece.reshape(groups, SUBLANES, LANES), axis=0)
            inverse_ref[m, 2 * q + half] = 1.0 / (1.0 + all_sublanes(total))

    def share(m, q):
        inverse = [inverse_ref[m, t] for t in range(chips)]
        for g in range(q * groups // slices, (q + 1) * groups // slices):
            rows = pl.ds(g * SUBLANES, SUBLANES)
            share_ref[m, rows] = added([weight_ref[m, t, rows] * inverse[t] for t in range(chips)])

    def predicted(m):
        return jnp.sum(share_ref[m].T, axis=0, keepdims=True) * (1.0 / R)

    def first_end(m):
        change = shares[m : m + 1] - jnp.log(predicted(m))
        factor = jnp.exp(change)
        row_ref[0, pl.ds(m, 1)] = change
        row_ref[1, pl.ds(m, 1)] = factor
        factor_ref[m] = jnp.broadcast_to(factor, (LANES, 2 * LANES)).T

    again = {}

    def weigh_again(m, q):
        totals = again.setdefault(m, [None] * chips)
        for g in range(q * groups // slices, (q + 1) * groups // slices):
            rows = pl.ds(g * SUBLANES, SUBLANES)
            scale = factor_ref[m, rows]
            for t in range(chips):
                term = weight_ref[m, t, rows] * scale
                totals[t] = term if totals[t] is None else totals[t] + term
        if q == slices - 1:
            for t in range(chips):
                inverse_ref[m, t] = 1.0 / (1.0 + all_sublanes(totals[t]))

    def second_end(m):
        row_ref[2, pl.ds(m, 1)] = predicted(m)

    for stage in range(markets + 3):
        a, b, c, d = (stage - lag if 0 <= stage - lag < markets else None for lag in range(4))
        if a is not None:
            left_of(a)
        for q in range(slices):
            if a is not None:
                weigh(a, q)
            if b is not None:
                share(b, q)
            if c is not None:
                weigh_again(c, q)
            if d is not None:
                share(d, q)
        if b is not None:
            first_end(b)
        if d is not None:
            second_end(d)

    first_change = row_ref[0]
    second_change = shares - jnp.log(row_ref[1] * row_ref[2])
    result = utility + first_change + second_change
    squares = []
    for change in (first_change, second_change):
        square = change * change
        square = square[:, :LANES] + square[:, LANES:]
        squares.append(jnp.sum(square, axis=0, keepdims=True))
    block = jnp.concatenate([result[:, :LANES], result[:, LANES:], first_rows(squares, SUBLANES)], axis=0)
    out_ref[...] = jnp.broadcast_to(block, (chips, 3 * SUBLANES, LANES))


def contraction(gate, coef_scale, own, other, taste):
    chips, markets, _, _ = taste.shape
    vmem = pl.BlockSpec(memory_space=pltpu.VMEM)
    return pl.pallas_call(
        contraction_kernel,
        out_shape=jax.ShapeDtypeStruct((chips, 3 * SUBLANES, LANES), jnp.float32),
        in_specs=[vmem] * 5,
        out_specs=vmem,
        scratch_shapes=[
            pltpu.VMEM((markets, chips, 2 * LANES, LANES), jnp.float32),
            pltpu.VMEM((markets, chips, SUBLANES, LANES), jnp.float32),
            pltpu.VMEM((markets, 2 * LANES, LANES), jnp.float32),
            pltpu.VMEM((markets, 2 * LANES, LANES), jnp.float32),
            pltpu.VMEM((markets, 4 * SUBLANES, 2 * LANES), jnp.bfloat16),
            pltpu.VMEM((3, markets, 2 * LANES), jnp.float32),
        ],
        compiler_params=pltpu.CompilerParams(vmem_limit_bytes=40 * 1024 * 1024),
    )(gate, coef_scale, own, other, taste)


def pick_kernel(utility_ref, shares_ref, chars_ref, coef_ref, taste_ref, half_ref, own_ref, given_ref, scale_ref, side_ref, sems):
    count = half_ref.shape[0]
    markets = own_ref.shape[0] - 2
    core, chip = lax.axis_index("prod"), lax.axis_index("draw")
    pairs = [(taste_ref.at[pl.ds(core * count, count)], half_ref), (coef_ref, scale_ref)]
    for ref, side in ((given_ref, 1 - core), (own_ref, core)):
        rows = pl.ds(side * count + chip * markets, markets)
        pairs.append((chars_ref.at[rows], ref.at[pl.ds(0, markets)]))
        pairs.append((utility_ref.at[rows], ref.at[markets]))
        pairs.append((shares_ref.at[rows], ref.at[markets + 1]))
    copies = [pltpu.make_async_copy(*pair, sems.at[i]) for i, pair in enumerate(pairs)]
    for copy in copies:
        copy.start()
    side_ref[...] = jnp.full(side_ref.shape, core, jnp.int32)
    for copy in copies:
        copy.wait()


def picked(utility, shares, chars, coef_scale, taste, count, markets):
    hbm = pl.BlockSpec(memory_space=pltpu.HBM)
    vmem = pl.BlockSpec(memory_space=pltpu.VMEM)
    packed = pltpu.VMEM((markets + 2, *chars.shape[1:]), chars.dtype)
    return pl.pallas_call(
        pick_kernel,
        out_shape=[pltpu.VMEM((count, *taste.shape[1:]), taste.dtype), packed, packed, pltpu.VMEM(coef_scale.shape, coef_scale.dtype), pltpu.VMEM((1, LANES), jnp.int32)],
        in_specs=[hbm] * 5,
        out_specs=[vmem] * 5,
        scratch_shapes=[pltpu.SemaphoreType.DMA((8,))],
    )(utility, shares, chars, coef_scale, taste)


def shards(start_utility, log_shares, characteristics, coef_scale, taste_draws):
    markets, coefs, _ = characteristics.shape
    cores, chips, planes = lax.axis_size("prod"), lax.axis_size("draw"), lax.axis_size("mkt")
    half = markets // cores
    own_markets = half // chips
    swap = [(0, 1), (1, 0)]

    taste, own, given, coef_scale, side = picked(start_utility, log_shares, characteristics, coef_scale, taste_draws, half, own_markets)
    other = lax.ppermute(given, "prod", swap)
    taste = lax.all_to_all(taste.reshape(chips, own_markets, coefs, LANES), "draw", 0, 0, tiled=True)
    gate = taste[0, 0] * 0.5
    blocks = contraction(gate, coef_scale, own, other, taste)
    blocks = lax.all_to_all(blocks, "draw", 0, 0, tiled=True)

    squares = jnp.sum(blocks[:, 2 * own_markets : 2 * own_markets + 2], axis=0)
    squares = jnp.broadcast_to(squares, (planes * cores, 2, LANES))
    squares = lax.all_to_all(squares, ("mkt", "prod"), 0, 0, tiled=True)
    given = blocks[:, own_markets : 2 * own_markets].reshape(half, LANES)
    given = lax.ppermute(given, "prod", swap)
    kept = blocks[:, :own_markets].reshape(half, LANES)
    first = side == 0
    utility = jnp.concatenate([jnp.where(first, kept, given), jnp.where(first, given, kept)], axis=0)
    cells = planes * markets * cores * LANES
    return utility, jnp.sqrt(jnp.sum(squares, axis=(0, 2)) / cells + 1e-06)


def solution(mesh):
    return jax.shard_map(
        shards,
        mesh=mesh,
        in_specs=(
            P("mkt", "prod"),
            P("mkt", "prod"),
            P("mkt", None, "prod"),
            P(),
            P("mkt", None, "draw"),
        ),
        out_specs=(P("mkt", "prod"), P()),
        check_vma=False,
    )
```

```python
import math

import jax
import jax.numpy as jnp
from jax import lax
from jax.experimental import pallas as pl
from jax.experimental.pallas import tpu as pltpu
from jax.sharding import PartitionSpec as P

R = 2048
LOG2E = math.log2(math.e)
LANES = 128
SUBLANES = 8


def rounded(x):
    return x.astype(jnp.bfloat16).astype(jnp.float32)


def first_rows(rows, length):
    width = rows[0].shape[-1]
    index = lax.broadcasted_iota(jnp.int32, (length, width), 0)
    out = jnp.zeros((length, width), jnp.float32)
    for position, row in enumerate(rows):
        out = jnp.where(index == position, jnp.broadcast_to(row, (length, width)), out)
    return out


def three_parts(x):
    high = rounded(x)
    middle = rounded(x - high)
    return high, middle, x - high - middle


def by_first(a, b):
    return lax.dot_general(a, b, (((0,), (0,)), ((), ())), preferred_element_type=jnp.float32)


def all_sublanes(x):
    for shift in (4, 2, 1):
        x = x + pltpu.roll(x, shift, 0)
    return x


def added(terms):
    while len(terms) > 1:
        terms = [a + b for a, b in zip(terms[::2], terms[1::2])]
    return terms[0]


def contraction_kernel(draws_ref, own_ref, other_ref, taste_ref, out_ref, weight_ref, inverse_ref, share_ref, factor_ref, left_ref, row_ref):
    coefs = 8
    markets = other_ref.shape[0] // (coefs + 2)
    chips = taste_ref.shape[0]
    groups = 2 * LANES // SUBLANES
    slices = chips // 2

    def part(first, count):
        return jnp.concatenate([own_ref[pl.ds(first, count)], other_ref[pl.ds(first, count)]], axis=1)

    coef = own_ref[pl.ds((coefs + 2) * markets, coefs)] * LOG2E
    coef = jnp.concatenate([coef, coef], axis=1)
    ones = first_rows([jnp.ones((1, 2 * LANES), jnp.float32)] * 3, SUBLANES)

    def left_of(m):
        chars = part(m * coefs, coefs) * coef
        high = rounded(chars)
        base = first_rows(three_parts(part(8 * markets + m, 1) * LOG2E), SUBLANES)
        left_ref[m] = jnp.concatenate([high, high, chars - high, base], axis=0).astype(jnp.bfloat16)

    def weigh(m, q):
        taste = jnp.concatenate([taste_ref[2 * q, m], taste_ref[2 * q + 1, m]], axis=1)
        taste_high = rounded(taste)
        right = jnp.concatenate([taste_high, taste - taste_high, taste_high, ones], axis=0).astype(jnp.bfloat16)
        weight = jnp.exp2(by_first(left_ref[m], right))
        for half in range(2):
            piece = weight[:, half * LANES : (half + 1) * LANES]
            weight_ref[m, 2 * q + half] = piece
            total = jnp.sum(piece.reshape(groups, SUBLANES, LANES), axis=0)
            inverse_ref[m, 2 * q + half] = 1.0 / (1.0 + all_sublanes(total))

    def share(m, q):
        inverse = [inverse_ref[m, t] for t in range(chips)]
        for g in range(q * groups // slices, (q + 1) * groups // slices):
            rows = pl.ds(g * SUBLANES, SUBLANES)
            share_ref[m, rows] = added([weight_ref[m, t, rows] * inverse[t] for t in range(chips)])

    def predicted(m):
        return jnp.sum(share_ref[m].T, axis=0, keepdims=True) * (1.0 / R)

    def first_end(m):
        change = part(9 * markets + m, 1) - jnp.log(predicted(m))
        factor = jnp.exp(change)
        row_ref[0, pl.ds(m, 1)] = change
        row_ref[1, pl.ds(m, 1)] = factor
        factor_ref[m] = jnp.broadcast_to(factor, (LANES, 2 * LANES)).T

    again = {}

    def weigh_again(m, q):
        totals = again.setdefault(m, [None] * chips)
        for g in range(q * groups // slices, (q + 1) * groups // slices):
            rows = pl.ds(g * SUBLANES, SUBLANES)
            scale = factor_ref[m, rows]
            for t in range(chips):
                term = weight_ref[m, t, rows] * scale
                totals[t] = term if totals[t] is None else totals[t] + term
        if q == slices - 1:
            for t in range(chips):
                inverse_ref[m, t] = 1.0 / (1.0 + all_sublanes(totals[t]))

    def second_end(m):
        row_ref[2, pl.ds(m, 1)] = predicted(m)

    for stage in range(markets + 3):
        a, b, c, d = (stage - lag if 0 <= stage - lag < markets else None for lag in range(4))
        if a is not None:
            left_of(a)
        for q in range(slices):
            if a is not None:
                weigh(a, q)
            if b is not None:
                share(b, q)
            if c is not None:
                weigh_again(c, q)
            if d is not None:
                share(d, q)
        if b is not None:
            first_end(b)
        if d is not None:
            second_end(d)

    first_change = row_ref[0]
    second_change = part(9 * markets, markets) - jnp.log(row_ref[1] * row_ref[2])
    result = part(8 * markets, markets) + first_change + second_change
    squares = []
    for change in (first_change, second_change):
        square = change * change
        square = square[:, :LANES] + square[:, LANES:]
        squares.append(jnp.sum(square, axis=0, keepdims=True))
    block = jnp.concatenate([result[:, :LANES], result[:, LANES:], first_rows(squares, SUBLANES)], axis=0)
    out_ref[...] = jnp.broadcast_to(block, (chips, 3 * SUBLANES, LANES))


def contraction(draws, own, other, taste):
    chips, markets, _, _ = taste.shape
    vmem = pl.BlockSpec(memory_space=pltpu.VMEM)
    return pl.pallas_call(
        contraction_kernel,
        out_shape=jax.ShapeDtypeStruct((chips, 3 * SUBLANES, LANES), jnp.float32),
        in_specs=[pl.BlockSpec(memory_space=pltpu.HBM), vmem, vmem, vmem],
        out_specs=vmem,
        scratch_shapes=[
            pltpu.VMEM((markets, chips, 2 * LANES, LANES), jnp.float32),
            pltpu.VMEM((markets, chips, SUBLANES, LANES), jnp.float32),
            pltpu.VMEM((markets, 2 * LANES, LANES), jnp.float32),
            pltpu.VMEM((markets, 2 * LANES, LANES), jnp.float32),
            pltpu.VMEM((markets, 4 * SUBLANES, 2 * LANES), jnp.bfloat16),
            pltpu.VMEM((3, markets, 2 * LANES), jnp.float32),
        ],
        compiler_params=pltpu.CompilerParams(vmem_limit_bytes=40 * 1024 * 1024),
    )(draws, own, other, taste)


def shards(start_utility, log_shares, characteristics, coef_scale, taste_draws):
    markets, coefs, _ = characteristics.shape
    cores, chips, planes = lax.axis_size("prod"), lax.axis_size("draw"), lax.axis_size("mkt")
    half = markets // cores
    own_markets = half // chips
    core, chip = (lax.axis_index(axis).astype(jnp.uint32) for axis in ("prod", "draw"))

    taste = lax.dynamic_slice_in_dim(taste_draws, core * half, half, 0).reshape(chips, own_markets, coefs, LANES)
    taste = lax.all_to_all(taste, "draw", 0, 0, tiled=True)

    def packed(first):
        chars = lax.dynamic_slice_in_dim(characteristics, first, own_markets, 0).reshape(-1, LANES)
        utility = lax.dynamic_slice_in_dim(start_utility, first, own_markets, 0)
        shares = lax.dynamic_slice_in_dim(log_shares, first, own_markets, 0)
        return jnp.concatenate([chars, utility, shares], axis=0)

    swap = [(0, 1), (1, 0)]
    scale = jnp.broadcast_to(coef_scale[:, None], (coefs, LANES))
    own = jnp.concatenate([packed(core * half + chip * own_markets), scale], axis=0)
    other = lax.ppermute(packed((1 - core) * half + chip * own_markets), "prod", swap)

    blocks = contraction(taste_draws, own, other, taste)
    blocks = lax.all_to_all(blocks, "draw", 0, 0, tiled=True)

    squares = jnp.sum(blocks[:, 2 * own_markets : 2 * own_markets + 2], axis=0)
    squares = jnp.broadcast_to(squares, (planes * cores, 2, LANES))
    squares = lax.all_to_all(squares, ("mkt", "prod"), 0, 0, tiled=True)
    kept = blocks[:, :own_markets].reshape(half, LANES)
    given = blocks[:, own_markets : 2 * own_markets].reshape(half, LANES)
    given = lax.ppermute(given, "prod", swap)
    utility = jnp.zeros((markets, LANES), jnp.float32)
    utility = lax.dynamic_update_slice_in_dim(utility, kept, core * half, 0)
    utility = lax.dynamic_update_slice_in_dim(utility, given, (1 - core) * half, 0)
    cells = planes * markets * cores * LANES
    return utility, jnp.sqrt(jnp.sum(squares, axis=(0, 2)) / cells + 1e-06)


def solution(mesh):
    return jax.shard_map(
        shards,
        mesh=mesh,
        in_specs=(
            P("mkt", "prod"),
            P("mkt", "prod"),
            P("mkt", None, "prod"),
            P(),
            P("mkt", None, "draw"),
        ),
        out_specs=(P("mkt", "prod"), P()),
        check_vma=False,
    )
```

```python
import math

import jax
import jax.numpy as jnp
from jax import lax
from jax.experimental import pallas as pl
from jax.experimental.pallas import tpu as pltpu
from jax.sharding import PartitionSpec as P

R = 2048
LOG2E = math.log2(math.e)
LANES = 128
SUBLANES = 8


FIRST_CHIP = 10
FIRST_PLACE = 8


def led_by(first, count):
    return [[(first + i) % count for i in range(count)]]


def rounded(x):
    return x.astype(jnp.bfloat16).astype(jnp.float32)


def first_rows(rows, length):
    width = rows[0].shape[-1]
    index = lax.broadcasted_iota(jnp.int32, (length, width), 0)
    out = jnp.zeros((length, width), jnp.float32)
    for position, row in enumerate(rows):
        out = jnp.where(index == position, jnp.broadcast_to(row, (length, width)), out)
    return out


def three_parts(x):
    high = rounded(x)
    middle = rounded(x - high)
    return high, middle, x - high - middle


def by_first(a, b):
    return lax.dot_general(a, b, (((0,), (0,)), ((), ())), preferred_element_type=jnp.float32)


def all_sublanes(x):
    for shift in (4, 2, 1):
        x = x + pltpu.roll(x, shift, 0)
    return x


def added(terms):
    while len(terms) > 1:
        terms = [a + b for a, b in zip(terms[::2], terms[1::2])]
    return terms[0]


def contraction_kernel(own_ref, other_ref, taste_ref, out_ref, weight_ref, inverse_ref, share_ref, factor_ref, left_ref, row_ref):
    coefs = 8
    markets = other_ref.shape[0] // (coefs + 2)
    chips = taste_ref.shape[0]
    groups = 2 * LANES // SUBLANES
    slices = chips // 2

    def part(first, count):
        return jnp.concatenate([own_ref[pl.ds(first, count)], other_ref[pl.ds(first, count)]], axis=1)

    coef = own_ref[pl.ds((coefs + 2) * markets, coefs)] * LOG2E
    coef = jnp.concatenate([coef, coef], axis=1)
    ones = first_rows([jnp.ones((1, 2 * LANES), jnp.float32)] * 3, SUBLANES)

    def left_of(m):
        chars = part(m * coefs, coefs) * coef
        high = rounded(chars)
        base = first_rows(three_parts(part(8 * markets + m, 1) * LOG2E), SUBLANES)
        left_ref[m] = jnp.concatenate([high, high, chars - high, base], axis=0).astype(jnp.bfloat16)

    def weigh(m, q):
        taste = jnp.concatenate([taste_ref[2 * q, m], taste_ref[2 * q + 1, m]], axis=1)
        taste_high = rounded(taste)
        right = jnp.concatenate([taste_high, taste - taste_high, taste_high, ones], axis=0).astype(jnp.bfloat16)
        weight = jnp.exp2(by_first(left_ref[m], right))
        for half in range(2):
            piece = weight[:, half * LANES : (half + 1) * LANES]
            weight_ref[m, 2 * q + half] = piece
            total = jnp.sum(piece.reshape(groups, SUBLANES, LANES), axis=0)
            inverse_ref[m, 2 * q + half] = 1.0 / (1.0 + all_sublanes(total))

    def share(m, q):
        inverse = [inverse_ref[m, t] for t in range(chips)]
        for g in range(q * groups // slices, (q + 1) * groups // slices):
            rows = pl.ds(g * SUBLANES, SUBLANES)
            share_ref[m, rows] = added([weight_ref[m, t, rows] * inverse[t] for t in range(chips)])

    def predicted(m):
        return jnp.sum(share_ref[m].T, axis=0, keepdims=True) * (1.0 / R)

    def first_end(m):
        change = part(9 * markets + m, 1) - jnp.log(predicted(m))
        factor = jnp.exp(change)
        row_ref[0, pl.ds(m, 1)] = change
        row_ref[1, pl.ds(m, 1)] = factor
        factor_ref[m] = jnp.broadcast_to(factor, (LANES, 2 * LANES)).T

    again = {}

    def weigh_again(m, q):
        totals = again.setdefault(m, [None] * chips)
        for g in range(q * groups // slices, (q + 1) * groups // slices):
            rows = pl.ds(g * SUBLANES, SUBLANES)
            scale = factor_ref[m, rows]
            for t in range(chips):
                term = weight_ref[m, t, rows] * scale
                totals[t] = term if totals[t] is None else totals[t] + term
        if q == slices - 1:
            for t in range(chips):
                inverse_ref[m, t] = 1.0 / (1.0 + all_sublanes(totals[t]))

    def second_end(m):
        row_ref[2, pl.ds(m, 1)] = predicted(m)

    for stage in range(markets + 3):
        a, b, c, d = (stage - lag if 0 <= stage - lag < markets else None for lag in range(4))
        if a is not None:
            left_of(a)
        for q in range(slices):
            if a is not None:
                weigh(a, q)
            if b is not None:
                share(b, q)
            if c is not None:
                weigh_again(c, q)
            if d is not None:
                share(d, q)
        if b is not None:
            first_end(b)
        if d is not None:
            second_end(d)

    first_change = row_ref[0]
    second_change = part(9 * markets, markets) - jnp.log(row_ref[1] * row_ref[2])
    result = part(8 * markets, markets) + first_change + second_change
    squares = []
    for change in (first_change, second_change):
        square = change * change
        square = square[:, :LANES] + square[:, LANES:]
        squares.append(jnp.sum(square, axis=0, keepdims=True))
    block = jnp.concatenate([result[:, :LANES], result[:, LANES:], first_rows(squares, SUBLANES)], axis=0)
    out_ref[...] = jnp.broadcast_to(block, (chips, 3 * SUBLANES, LANES))


def contraction(own, other, taste):
    chips, markets, _, _ = taste.shape
    vmem = pl.BlockSpec(memory_space=pltpu.VMEM)
    return pl.pallas_call(
        contraction_kernel,
        out_shape=jax.ShapeDtypeStruct((chips, 3 * SUBLANES, LANES), jnp.float32),
        in_specs=[vmem, vmem, vmem],
        out_specs=vmem,
        scratch_shapes=[
            pltpu.VMEM((markets, chips, 2 * LANES, LANES), jnp.float32),
            pltpu.VMEM((markets, chips, SUBLANES, LANES), jnp.float32),
            pltpu.VMEM((markets, 2 * LANES, LANES), jnp.float32),
            pltpu.VMEM((markets, 2 * LANES, LANES), jnp.float32),
            pltpu.VMEM((markets, 4 * SUBLANES, 2 * LANES), jnp.bfloat16),
            pltpu.VMEM((3, markets, 2 * LANES), jnp.float32),
        ],
        compiler_params=pltpu.CompilerParams(vmem_limit_bytes=40 * 1024 * 1024),
    )(own, other, taste)


def take_half_kernel(whole_ref, half_ref, staging_ref, read_sems, write_sems):
    pieces = read_sems.shape[0]
    count = half_ref.shape[0]
    size = count // pieces
    first = lax.axis_index("prod") * count

    def read(i):
        return pltpu.make_async_copy(whole_ref.at[pl.ds(first + i * size, size)], staging_ref.at[pl.ds(i * size, size)], read_sems.at[i])

    def write(i):
        return pltpu.make_async_copy(staging_ref.at[pl.ds(i * size, size)], half_ref.at[pl.ds(i * size, size)], write_sems.at[i])

    for i in range(pieces):
        read(i).start()
    for i in range(pieces):
        read(i).wait()
        write(i).start()
    for i in range(pieces):
        write(i).wait()


def take_half(whole, count):
    shape = (count, *whole.shape[1:])
    hbm = pl.BlockSpec(memory_space=pltpu.HBM)
    return pl.pallas_call(
        take_half_kernel,
        out_shape=jax.ShapeDtypeStruct(shape, whole.dtype),
        in_specs=[hbm],
        out_specs=hbm,
        scratch_shapes=[pltpu.VMEM(shape, whole.dtype), pltpu.SemaphoreType.DMA((4,)), pltpu.SemaphoreType.DMA((4,))],
    )(whole)


def shards(start_utility, log_shares, characteristics, coef_scale, taste_draws):
    markets, coefs, _ = characteristics.shape
    cores, chips, planes = lax.axis_size("prod"), lax.axis_size("draw"), lax.axis_size("mkt")
    half = markets // cores
    own_markets = half // chips
    core, chip = (lax.axis_index(axis).astype(jnp.uint32) for axis in ("prod", "draw"))
    plane, meeting = led_by(FIRST_CHIP, chips), led_by(FIRST_PLACE, planes * cores)
    chip = (chip + chips - FIRST_CHIP) % chips

    taste = take_half(taste_draws, half).reshape(chips, own_markets, coefs, LANES)
    taste = lax.all_to_all(taste, "draw", 0, 0, axis_index_groups=plane, tiled=True)

    def packed(first):
        chars = lax.dynamic_slice_in_dim(characteristics, first, own_markets, 0).reshape(-1, LANES)
        utility = lax.dynamic_slice_in_dim(start_utility, first, own_markets, 0)
        shares = lax.dynamic_slice_in_dim(log_shares, first, own_markets, 0)
        return jnp.concatenate([chars, utility, shares], axis=0)

    swap = [(0, 1), (1, 0)]
    scale = jnp.broadcast_to(coef_scale[:, None], (coefs, LANES))
    own = jnp.concatenate([packed(core * half + chip * own_markets), scale], axis=0)
    other = lax.ppermute(packed((1 - core) * half + chip * own_markets), "prod", swap)

    blocks = contraction(own, other, taste)
    blocks = lax.all_to_all(blocks, "draw", 0, 0, axis_index_groups=plane, tiled=True)

    squares = jnp.sum(blocks[:, 2 * own_markets : 2 * own_markets + 2], axis=0)
    squares = jnp.broadcast_to(squares, (planes * cores, 2, LANES))
    squares = lax.all_to_all(squares, ("mkt", "prod"), 0, 0, axis_index_groups=meeting, tiled=True)
    kept = blocks[:, :own_markets].reshape(half, LANES)
    given = blocks[:, own_markets : 2 * own_markets].reshape(half, LANES)
    given = lax.ppermute(given, "prod", swap)
    utility = jnp.zeros((markets, LANES), jnp.float32)
    utility = lax.dynamic_update_slice_in_dim(utility, kept, core * half, 0)
    utility = lax.dynamic_update_slice_in_dim(utility, given, (1 - core) * half, 0)
    cells = planes * markets * cores * LANES
    return utility, jnp.sqrt(jnp.sum(squares, axis=(0, 2)) / cells + 1e-06)


def solution(mesh):
    return jax.shard_map(
        shards,
        mesh=mesh,
        in_specs=(
            P("mkt", "prod"),
            P("mkt", "prod"),
            P("mkt", None, "prod"),
            P(),
            P("mkt", None, "draw"),
        ),
        out_specs=(P("mkt", "prod"), P()),
        check_vma=False,
    )
```

```python
import math

import jax
import jax.numpy as jnp
from jax import lax
from jax.experimental import pallas as pl
from jax.experimental.pallas import tpu as pltpu
from jax.sharding import PartitionSpec as P

R = 2048
LOG2E = math.log2(math.e)
LANES = 128
SUBLANES = 8


FIRST_CHIP = 10
FIRST_PLACE = 11


def led_by(first, count):
    return [[(first + i) % count for i in range(count)]]


def rounded(x):
    return x.astype(jnp.bfloat16).astype(jnp.float32)


def first_rows(rows, length):
    width = rows[0].shape[-1]
    index = lax.broadcasted_iota(jnp.int32, (length, width), 0)
    out = jnp.zeros((length, width), jnp.float32)
    for position, row in enumerate(rows):
        out = jnp.where(index == position, jnp.broadcast_to(row, (length, width)), out)
    return out


def three_parts(x):
    high = rounded(x)
    middle = rounded(x - high)
    return high, middle, x - high - middle


def by_first(a, b):
    return lax.dot_general(a, b, (((0,), (0,)), ((), ())), preferred_element_type=jnp.float32)


def all_sublanes(x):
    for shift in (4, 2, 1):
        x = x + pltpu.roll(x, shift, 0)
    return x


def added(terms):
    while len(terms) > 1:
        terms = [a + b for a, b in zip(terms[::2], terms[1::2])]
    return terms[0]


def contraction_kernel(gate_ref, coef_ref, own_ref, other_ref, taste_ref, out_ref, weight_ref, inverse_ref, share_ref, factor_ref, left_ref, row_ref):
    coefs = own_ref.shape[1]
    markets = own_ref.shape[0] - 2
    chips = taste_ref.shape[0]
    groups = 2 * LANES // SUBLANES
    slices = chips // 2

    def part(i):
        return jnp.concatenate([own_ref[i], other_ref[i]], axis=1)

    utility, shares = part(markets), part(markets + 1)
    square = (coefs, coefs)
    diagonal = lax.broadcasted_iota(jnp.int32, square, 0) == lax.broadcasted_iota(jnp.int32, square, 1)
    coef = jnp.where(diagonal, jnp.broadcast_to(coef_ref[...].reshape(1, coefs), square), 0.0)
    coef = jnp.broadcast_to(jnp.sum(coef, axis=1, keepdims=True) * LOG2E, (coefs, 2 * LANES))
    ones = first_rows([jnp.ones((1, 2 * LANES), jnp.float32)] * 3, SUBLANES)

    def left_of(m):
        chars = part(m) * coef
        high = rounded(chars)
        base = first_rows(three_parts(utility[m : m + 1] * LOG2E), SUBLANES)
        left_ref[m] = jnp.concatenate([high, high, chars - high, base], axis=0).astype(jnp.bfloat16)

    def weigh(m, q):
        taste = jnp.concatenate([taste_ref[2 * q, m], taste_ref[2 * q + 1, m]], axis=1)
        taste_high = rounded(taste)
        right = jnp.concatenate([taste_high, taste - taste_high, taste_high, ones], axis=0).astype(jnp.bfloat16)
        weight = jnp.exp2(by_first(left_ref[m], right))
        for half in range(2):
            piece = weight[:, half * LANES : (half + 1) * LANES]
            weight_ref[m, 2 * q + half] = piece
            total = jnp.sum(piece.reshape(groups, SUBLANES, LANES), axis=0)
            inverse_ref[m, 2 * q + half] = 1.0 / (1.0 + all_sublanes(total))

    def share(m, q):
        inverse = [inverse_ref[m, t] for t in range(chips)]
        for g in range(q * groups // slices, (q + 1) * groups // slices):
            rows = pl.ds(g * SUBLANES, SUBLANES)
            share_ref[m, rows] = added([weight_ref[m, t, rows] * inverse[t] for t in range(chips)])

    def predicted(m):
        return jnp.sum(share_ref[m].T, axis=0, keepdims=True) * (1.0 / R)

    def first_end(m):
        change = shares[m : m + 1] - jnp.log(predicted(m))
        factor = jnp.exp(change)
        row_ref[0, pl.ds(m, 1)] = change
        row_ref[1, pl.ds(m, 1)] = factor
        factor_ref[m] = jnp.broadcast_to(factor, (LANES, 2 * LANES)).T

    again = {}

    def weigh_again(m, q):
        totals = again.setdefault(m, [None] * chips)
        for g in range(q * groups // slices, (q + 1) * groups // slices):
            rows = pl.ds(g * SUBLANES, SUBLANES)
            scale = factor_ref[m, rows]
            for t in range(chips):
                term = weight_ref[m, t, rows] * scale
                totals[t] = term if totals[t] is None else totals[t] + term
        if q == slices - 1:
            for t in range(chips):
                inverse_ref[m, t] = 1.0 / (1.0 + all_sublanes(totals[t]))

    def second_end(m):
        row_ref[2, pl.ds(m, 1)] = predicted(m)

    for stage in range(markets + 3):
        a, b, c, d = (stage - lag if 0 <= stage - lag < markets else None for lag in range(4))
        if a is not None:
            left_of(a)
        for q in range(slices):
            if a is not None:
                weigh(a, q)
            if b is not None:
                share(b, q)
            if c is not None:
                weigh_again(c, q)
            if d is not None:
                share(d, q)
        if b is not None:
            first_end(b)
        if d is not None:
            second_end(d)

    first_change = row_ref[0]
    second_change = shares - jnp.log(row_ref[1] * row_ref[2])
    result = utility + first_change + second_change
    squares = []
    for change in (first_change, second_change):
        square = change * change
        square = square[:, :LANES] + square[:, LANES:]
        squares.append(jnp.sum(square, axis=0, keepdims=True))
    block = jnp.concatenate([result[:, :LANES], result[:, LANES:], first_rows(squares, SUBLANES)], axis=0)
    out_ref[...] = jnp.broadcast_to(block, (chips, 3 * SUBLANES, LANES))


def contraction(gate, coef_scale, own, other, taste):
    chips, markets, _, _ = taste.shape
    vmem = pl.BlockSpec(memory_space=pltpu.VMEM)
    return pl.pallas_call(
        contraction_kernel,
        out_shape=jax.ShapeDtypeStruct((chips, 3 * SUBLANES, LANES), jnp.float32),
        in_specs=[vmem] * 5,
        out_specs=vmem,
        scratch_shapes=[
            pltpu.VMEM((markets, chips, 2 * LANES, LANES), jnp.float32),
            pltpu.VMEM((markets, chips, SUBLANES, LANES), jnp.float32),
            pltpu.VMEM((markets, 2 * LANES, LANES), jnp.float32),
            pltpu.VMEM((markets, 2 * LANES, LANES), jnp.float32),
            pltpu.VMEM((markets, 4 * SUBLANES, 2 * LANES), jnp.bfloat16),
            pltpu.VMEM((3, markets, 2 * LANES), jnp.float32),
        ],
        compiler_params=pltpu.CompilerParams(vmem_limit_bytes=40 * 1024 * 1024),
    )(gate, coef_scale, own, other, taste)


def pick_kernel(utility_ref, shares_ref, chars_ref, coef_ref, taste_ref, half_ref, own_ref, given_ref, scale_ref, side_ref, sems):
    count = half_ref.shape[0]
    markets = own_ref.shape[0] - 2
    core = lax.axis_index("prod")
    chips = lax.axis_size("draw")
    chip = (lax.axis_index("draw") + (chips - FIRST_CHIP)) % chips
    pairs = [(taste_ref.at[pl.ds(core * count, count)], half_ref), (coef_ref, scale_ref)]
    for ref, side in ((given_ref, 1 - core), (own_ref, core)):
        rows = pl.ds(side * count + chip * markets, markets)
        pairs.append((chars_ref.at[rows], ref.at[pl.ds(0, markets)]))
        pairs.append((utility_ref.at[rows], ref.at[markets]))
        pairs.append((shares_ref.at[rows], ref.at[markets + 1]))
    copies = [pltpu.make_async_copy(*pair, sems.at[i]) for i, pair in enumerate(pairs)]
    for copy in copies:
        copy.start()
    side_ref[...] = jnp.full(side_ref.shape, core, jnp.int32)
    for copy in copies:
        copy.wait()


def picked(utility, shares, chars, coef_scale, taste, count, markets):
    hbm = pl.BlockSpec(memory_space=pltpu.HBM)
    vmem = pl.BlockSpec(memory_space=pltpu.VMEM)
    packed = pltpu.VMEM((markets + 2, *chars.shape[1:]), chars.dtype)
    return pl.pallas_call(
        pick_kernel,
        out_shape=[pltpu.VMEM((count, *taste.shape[1:]), taste.dtype), packed, packed, pltpu.VMEM(coef_scale.shape, coef_scale.dtype), pltpu.VMEM((1, LANES), jnp.int32)],
        in_specs=[hbm] * 5,
        out_specs=[vmem] * 5,
        scratch_shapes=[pltpu.SemaphoreType.DMA((8,))],
    )(utility, shares, chars, coef_scale, taste)


def shards(start_utility, log_shares, characteristics, coef_scale, taste_draws):
    markets, coefs, _ = characteristics.shape
    cores, chips, planes = lax.axis_size("prod"), lax.axis_size("draw"), lax.axis_size("mkt")
    half = markets // cores
    own_markets = half // chips
    swap = [(0, 1), (1, 0)]
    plane, meeting = led_by(FIRST_CHIP, chips), led_by(FIRST_PLACE, planes * cores)

    taste, own, given, coef_scale, side = picked(start_utility, log_shares, characteristics, coef_scale, taste_draws, half, own_markets)
    other = lax.ppermute(given, "prod", swap)
    taste = lax.all_to_all(taste.reshape(chips, own_markets, coefs, LANES), "draw", 0, 0, axis_index_groups=plane, tiled=True)
    gate = taste[0, 0] * 0.5
    blocks = contraction(gate, coef_scale, own, other, taste)
    blocks = lax.all_to_all(blocks, "draw", 0, 0, axis_index_groups=plane, tiled=True)

    squares = jnp.sum(blocks[:, 2 * own_markets : 2 * own_markets + 2], axis=0)
    squares = jnp.broadcast_to(squares, (planes * cores, 2, LANES))
    squares = lax.all_to_all(squares, ("mkt", "prod"), 0, 0, axis_index_groups=meeting, tiled=True)
    given = blocks[:, own_markets : 2 * own_markets].reshape(half, LANES)
    given = lax.ppermute(given, "prod", swap)
    kept = blocks[:, :own_markets].reshape(half, LANES)
    first = side == 0
    utility = jnp.concatenate([jnp.where(first, kept, given), jnp.where(first, given, kept)], axis=0)
    cells = planes * markets * cores * LANES
    return utility, jnp.sqrt(jnp.sum(squares, axis=(0, 2)) / cells + 1e-06)


def solution(mesh):
    return jax.shard_map(
        shards,
        mesh=mesh,
        in_specs=(
            P("mkt", "prod"),
            P("mkt", "prod"),
            P("mkt", None, "prod"),
            P(),
            P("mkt", None, "draw"),
        ),
        out_specs=(P("mkt", "prod"), P()),
        check_vma=False,
    )
```
